32 devices in a mesh: lat: 8 (over y, x, core), lon: 4 (over z).
Axes of the slice: x: 2, y: 2, z: 4, core: 2. Of those that a mesh axis runs over, the one named last changes fastest.
Arguments:
- coeffs_old: float32 [640, 2, 3, 50, 640], P(('lat', 'lon')), may hold values from -0.16 to 0.16
- noise: bfloat16 [640, 2, 3, 50, 640], P(('lat', 'lon')), may hold values from -6 to 6
- legendre: float32 [640, 640, 640], P(('lat', 'lon')), may hold values from -0.25 to 0.25
- decay: float32 [3], replicated, may hold values from 0.3 to 0.97
- amplitude: float32 [3, 640], replicated, may hold values from 0.005 to 0.05
- wavenumber_of_slot: int32 [640], replicated, may hold values from 0 to 639, as said below
- lat_order: int32 [640], replicated, may hold values from 0 to 639, each once
Outputs:
- coeffs_new: float32 [640, 2, 3, 50, 640], P(('lat', 'lon'))
- pattern: float32 [640, 50, 1280], P(('lat', 'lon'))
The draws below stay inside these ranges and needn't reach their ends.
Inputs may be any that keep to these rules, and one draw needn't show every extreme that they name: `wavenumber_of_slot`: every wavenumber fills exactly one slot; the sums of the wavenumbers of one device's 20 slots differ between devices by less than 32. `lat_order`: every latitude stands in exactly one row.
All inputs are finite; a program needn't handle non-finite values.
Results may differ from the reference program's by a relative error of at most 0.0003.
Values sent between devices are 32-bit elements; how exact they have to be, the bound alone decides.
No kernel may reach another device: no remote copies, remote signals or barrier semaphores. Data moves between devices by JAX's collectives and lax.ppermute only.
A program may use at most 192 MiB of HBM per device.

```python
import math
import jax
import jax.numpy as jnp
from jax import lax

M = 640
LAT = 640
LON = 1280
SCALES = 3
MEMBERS = 50
SLOT_DEV = 20


def draw_wavenumber_of_slot(key, part):
    devices_all = M // SLOT_DEV
    position = jax.random.permutation(jax.random.fold_in(key, 11), devices_all).astype(jnp.int32)
    rounds = jnp.arange(SLOT_DEV, dtype=jnp.int32)
    dealt = jnp.where(rounds[None, :] % 2 == 0, position[:, None], devices_all - 1 - position[:, None])
    table = rounds[None, :] * devices_all + dealt
    return table.reshape(-1).astype(jnp.int32)


def shard_levels(stream_key, shape, cuts, low, high):
    def one(dim, blocks):
        steps = jax.random.uniform(jax.random.fold_in(jax.random.fold_in(stream_key, 6), dim), (blocks,), jnp.float32, low / len(cuts), high / len(cuts))
        return jnp.repeat(jnp.exp(steps), shape[dim] // blocks).reshape((-1,) + (1,) * (len(shape) - dim - 1))

    loudness = one(*cuts[0])
    for cut in cuts[1:]:
        loudness = loudness * one(*cut)
    return loudness


def scatter_about(own_key, dims, scale, bound, shards=(), kind=jnp.bfloat16):
    result = scale * jax.random.normal(own_key, dims, jnp.float32)
    if shards:
        result = result * shard_levels(own_key, dims, shards, -0.22, 0.18)
    return jnp.clip(result, -bound, bound).astype(kind)


def setup_inputs(seed: int = 0) -> dict:
    arg_keys = jax.random.split(jax.random.key(seed), 8)
    coeffs_old = scatter_about(arg_keys[0], (M, 2, SCALES, MEMBERS, M), 0.02, 0.16, ((0, 32),), jnp.float32)
    noise = scatter_about(arg_keys[1], (M, 2, SCALES, MEMBERS, M), 1.0, 6.0, ((0, 32),))
    legendre = scatter_about(arg_keys[2], (M, LAT, M), M ** -0.5, 0.25, ((0, 32),), jnp.float32)
    decay = jnp.clip(jax.random.uniform(arg_keys[3], (SCALES,), jnp.float32, 0.3, 0.97), 0.3, 0.97)
    amplitude = jnp.clip(jnp.exp(jax.random.uniform(arg_keys[4], (SCALES, M), jnp.float32, math.log(0.005), math.log(0.05))), 0.005, 0.05)
    wavenumber_of_slot = draw_wavenumber_of_slot(jax.random.fold_in(arg_keys[7], 71), 0)
    lat_order = jax.random.permutation(arg_keys[6], LAT).astype(jnp.int32)
    return {"coeffs_old": coeffs_old, "noise": noise, "legendre": legendre, "decay": decay, "amplitude": amplitude, "wavenumber_of_slot": wavenumber_of_slot, "lat_order": lat_order}


def evolve(coeffs_old, noise, decay, amplitude, waves):
    width = coeffs_old.shape[4]
    offsets = lax.broadcasted_iota(jnp.int32, (waves.shape[0], width), 1)
    live = waves[:, None] + offsets < width
    padded = jnp.concatenate([amplitude, jnp.zeros_like(amplitude)], axis=1)
    spread = jax.vmap(lambda wave: lax.dynamic_slice_in_dim(padded, wave, width, 1))(waves)
    factor = jnp.sqrt(1.0 - decay * decay)
    fresh = decay[None, None, :, None, None] * coeffs_old + (spread * factor[None, :, None])[:, None, :, None, :] * noise.astype(jnp.float32)
    return jnp.where(live[:, None, None, None, :], fresh, jnp.zeros_like(fresh))

def reference(coeffs_old, noise, legendre, decay, amplitude, wavenumber_of_slot, lat_order):
    waves = wavenumber_of_slot.astype(jnp.int32)
    coeffs_new = evolve(coeffs_old, noise, decay, amplitude, waves)

    def per_slot(pair):
        coeff, basis = pair
        return jnp.einsum('rkej,lj->rel', coeff, basis, precision=lax.Precision.HIGHEST)
    field = lax.map(per_slot, (coeffs_new, legendre))
    real_part = jnp.zeros((M,) + field.shape[2:], field.dtype).at[waves].set(field[:, 0])
    imag_part = jnp.zeros((M,) + field.shape[2:], field.dtype).at[waves].set(field[:, 1])
    positive = jnp.arange(M, dtype=jnp.int32)[:, None, None] > 0
    imag_part = jnp.where(positive, imag_part, jnp.zeros_like(imag_part))
    real_part = jnp.take(real_part, lat_order.astype(jnp.int32), axis=2)
    imag_part = jnp.take(imag_part, lat_order.astype(jnp.int32), axis=2)
    spectrum = real_part + 1j * imag_part
    grid = jnp.fft.irfft(spectrum, n=LON, axis=0) * LON
    pattern = jnp.transpose(grid, (2, 1, 0))
    return (coeffs_new, pattern)
```

```python
import jax
import jax.numpy as jnp
from jax import lax
from jax.experimental import pallas as pl
from jax.experimental.pallas import tpu as pltpu
from jax.sharding import PartitionSpec as P

TWO_PI = 6.283185307179586
LON = 1280
LANES = 128
AXES = ("lat", "lon")


def chunks_of(slots):
    if slots % 4:
        return (slots,)
    if slots >= 16:
        return (4, slots - 8, 4)
    return (slots,)


def round_up(value, unit):
    return -(-value // unit) * unit


def spectral_kernel(
    first, slots, count, groups, group_rows, members, rows_p, waves, decay, old, noise,
    legendre, drive, select, *rest
):
    if first:
        base = 0
    else:
        base = 1
    new = rest[base]
    outs = rest[base + 1 : base + 1 + count]
    drive_rows, total, spectrum, packed = rest[base + 1 + count :]
    scales = old.shape[1]
    width = old.shape[4]
    step = pl.program_id(0)
    half = spectrum.shape[0] // 4
    blocks = count * groups

    @pl.when(step == 0)
    def _():
        spectrum[...] = jnp.zeros_like(spectrum)
        if rows_p != 2 * slots:
            packed[...] = jnp.zeros_like(packed)

    wave = waves[step]
    live_row = lax.broadcasted_iota(jnp.int32, (1, 2, width), 2) + wave < width
    rolled = pltpu.roll(drive[...], lax.rem(width - wave, width), 1)
    for k in range(scales):
        drive_rows[k] = jnp.broadcast_to(rolled[k : k + 1], (2, width))
    sums = None
    for k in range(scales):
        keep = jnp.where(live_row, decay[k], 0.0)
        gain = jnp.where(live_row, drive_rows[k][None], 0.0)
        fresh = keep * old[0, k] + gain * noise[0, k].astype(jnp.float32)
        new[0, k] = fresh
        sums = fresh if sums is None else sums + fresh
    total[...] = sums
    for r in range(2):
        part = total[:, r, :]
        high = part.astype(jnp.bfloat16)
        low = (part - high.astype(jnp.float32)).astype(jnp.bfloat16)
        spectrum[r * half : r * half + members] = high
        spectrum[(2 + r) * half : (2 + r) * half + members] = low
    basis = legendre[0]
    basis_high = basis.astype(jnp.bfloat16)
    basis_low = (basis - basis_high.astype(jnp.float32)).astype(jnp.bfloat16)
    nt = (((1,), (1,)), ((), ()))
    wide = lax.dot_general(basis_high, spectrum[...], nt, preferred_element_type=jnp.float32)
    narrow = lax.dot_general(
        basis_low, spectrum[: 2 * half], nt, preferred_element_type=jnp.float32
    )
    field = wide[:, : 2 * half] + wide[:, 2 * half :] + narrow
    field_high = field.astype(jnp.bfloat16)
    field_low = (field - field_high.astype(jnp.float32)).astype(jnp.bfloat16)
    both = jnp.dot(
        select[...],
        jnp.concatenate([field_high, field_low], axis=1),
        preferred_element_type=jnp.float32,
    )
    chosen = both[:, : 2 * half] + both[:, 2 * half :]
    lane = lax.broadcasted_iota(jnp.int32, (blocks, LANES), 1)
    for r in range(2):
        tiles = [jnp.zeros((blocks, LANES), jnp.float32) for _ in range(2)]
        for i in range(group_rows):
            start = i * members
            piece = chosen[i * blocks : (i + 1) * blocks]
            shift = (start - r * half) % LANES
            if shift:
                piece = pltpu.roll(piece, shift, 1)
            for tile in range(2):
                begin = max(start - tile * LANES, 0)
                end = min(start + members - tile * LANES, LANES)
                if begin < end:
                    tiles[tile] = jnp.where((lane >= begin) & (lane < end), piece, tiles[tile])
        for tile in range(2):
            packed[pl.ds(tile * rows_p + 2 * step + r, blocks, stride=2 * rows_p), :] = tiles[tile]

    @pl.when(step == slots - 1)
    def _():
        size = groups * 2 * rows_p
        for d in range(count):
            outs[d][...] = packed[d * size : (d + 1) * size]


def spectral(old, noise, legendre, drive, decay, waves, select, start, slots, previous, count, groups, group_rows):
    members = old.shape[2]
    scales = old.shape[1]
    width = old.shape[4]
    rows_p = round_up(2 * slots, 8)
    first = previous is None
    size = groups * 2 * rows_p

    def body(*refs):
        spectral_kernel(first, slots, count, groups, group_rows, members, rows_p, *refs)

    state = pl.BlockSpec((1, scales, members, 2, width), lambda i: (start + i, 0, 0, 0, 0))
    in_specs = [
        pl.BlockSpec(memory_space=pltpu.SMEM),
        pl.BlockSpec(memory_space=pltpu.SMEM),
        state,
        state,
        pl.BlockSpec((1,) + legendre.shape[1:], lambda i: (start + i, 0, 0)),
        pl.BlockSpec(drive.shape, lambda i: (0, 0)),
        pl.BlockSpec(select.shape, lambda i: (0, 0)),
    ]
    args = [lax.slice_in_dim(waves, start, start + slots), decay, old, noise, legendre, drive, select]
    aliases = {}
    if not first:
        in_specs.append(pl.BlockSpec(memory_space=pl.ANY))
        aliases = {len(args): 0}
        args.append(previous)
    message = jax.ShapeDtypeStruct((size, LANES), jnp.float32)
    result = pl.pallas_call(
        body,
        grid=(slots,),
        in_specs=in_specs,
        out_specs=[state] + [pl.BlockSpec((size, LANES), lambda i: (0, 0))] * count,
        out_shape=[jax.ShapeDtypeStruct(old.shape, jnp.float32)] + [message] * count,
        scratch_shapes=[
            pltpu.VMEM((scales, 2, width), jnp.float32),
            pltpu.VMEM((members, 2, width), jnp.float32),
            pltpu.VMEM((4 * 64, width), jnp.bfloat16),
            pltpu.VMEM((count * size, LANES), jnp.float32),
        ],
        input_output_aliases=aliases,
        compiler_params=pltpu.CompilerParams(dimension_semantics=("arbitrary",)),
        cost_estimate=pl.CostEstimate(
            flops=slots * 2 * 10**9 // 4, bytes_accessed=slots * 3500000, transcendentals=0
        ),
        name="spectral",
    )(*args)
    return result[0], result[1:]


def synthesis_kernel(has_previous, final, count, rows_p, members, group_rows, table, *rest):
    sources = rest[:count]
    rest = rest[count:]
    previous = None
    if has_previous:
        previous = rest[0]
        rest = rest[1:]
    out, table_high, table_low, stack = rest
    group = pl.program_id(0)

    @pl.when(group == 0)
    def _():
        values = table[...]
        high = values.astype(jnp.bfloat16)
        table_high[...] = high
        table_low[...] = (values - high.astype(jnp.float32)).astype(jnp.bfloat16)

    for d in range(count):
        for tile in range(2):
            offset = pl.multiple_of((group * 2 + tile) * rows_p, 8)
            stack[d * rows_p : (d + 1) * rows_p, tile * LANES : (tile + 1) * LANES] = sources[d][
                pl.ds(offset, rows_p), :
            ]
    turned = stack[...].T
    high = turned.astype(jnp.bfloat16)
    low = (turned - high.astype(jnp.float32)).astype(jnp.bfloat16)
    result = jnp.dot(high, table_high[...], preferred_element_type=jnp.float32)
    result += jnp.dot(low, table_high[...], preferred_element_type=jnp.float32)
    result += jnp.dot(high, table_low[...], preferred_element_type=jnp.float32)
    if has_previous:
        result += previous[0]
    if final:
        for i in range(group_rows):
            out[i] = result[i * members : (i + 1) * members]
    else:
        out[0] = result


def synthesis(table, sources, previous, final, groups, group_rows, members):
    count = len(sources)
    rows_p = table.shape[0] // count
    length = table.shape[1]

    def body(*refs):
        synthesis_kernel(previous is not None, final, count, rows_p, members, group_rows, *refs)

    in_specs = [pl.BlockSpec(table.shape, lambda g: (0, 0))]
    in_specs += [pl.BlockSpec(s.shape, lambda g: (0, 0)) for s in sources]
    args = [table, *sources]
    partial = pl.BlockSpec((1, 2 * LANES, length), lambda g: (g, 0, 0))
    aliases = {}
    if previous is not None:
        in_specs.append(partial)
        if not final:
            aliases = {len(args): 0}
        args.append(previous)
    if final:
        out_spec = pl.BlockSpec((group_rows, members, length), lambda g: (g, 0, 0))
        out_shape = jax.ShapeDtypeStruct((groups * group_rows, members, length), jnp.float32)
    else:
        out_spec = partial
        out_shape = jax.ShapeDtypeStruct((groups, 2 * LANES, length), jnp.float32)
    return pl.pallas_call(
        body,
        grid=(groups,),
        in_specs=in_specs,
        out_specs=out_spec,
        out_shape=out_shape,
        scratch_shapes=[
            pltpu.VMEM(table.shape, jnp.bfloat16),
            pltpu.VMEM(table.shape, jnp.bfloat16),
            pltpu.VMEM((table.shape[0], 2 * LANES), jnp.float32),
        ],
        input_output_aliases=aliases,
        compiler_params=pltpu.CompilerParams(dimension_semantics=("arbitrary",)),
        cost_estimate=pl.CostEstimate(
            flops=6 * groups * 256 * table.shape[0] * length, bytes_accessed=12 * 10**6, transcendentals=0
        ),
        name="synthesis",
    )(*args)


def by_offset(values, me):
    count = values.shape[0]
    ids = lax.broadcasted_iota(jnp.int32, (count, count, 1), 0) ^ me
    others = lax.broadcasted_iota(jnp.int32, (count, count, 1), 1)
    return jnp.sum(jnp.where(ids == others, values[None], 0), axis=1)


def synthesis_table(waves, rows_p, length):
    count, slots = waves.shape
    column = lax.broadcasted_iota(jnp.int32, (count, slots, 1, length), 3)
    wave = waves[:, :, None, None]
    part = lax.broadcasted_iota(jnp.int32, (count, slots, 2, length), 2)
    angle = (wave * column % length).astype(jnp.float32) * (TWO_PI / length)
    weight = jnp.where(wave == 0, 1.0, 2.0).astype(jnp.float32)
    table = jnp.where(part == 0, weight * jnp.cos(angle), -weight * jnp.sin(angle))
    table = table.reshape(count, 2 * slots, length)
    if rows_p != 2 * slots:
        table = jnp.pad(table, ((0, 0), (0, rows_p - 2 * slots), (0, 0)))
    return table.reshape(count * rows_p, length)


def local(coeffs_old, noise, legendre, decay, amplitude, wavenumber_of_slot, lat_order):
    lat_count = lax.axis_size("lat")
    lon_count = lax.axis_size("lon")
    count = lat_count * lon_count
    me = lax.axis_index("lat") * lon_count + lax.axis_index("lon")
    slots, _, scales, members, width = coeffs_old.shape
    latitudes = lat_order.shape[0]
    rows = latitudes // count
    group_rows = (2 * LANES) // members
    while rows % group_rows:
        group_rows -= 1
    groups = rows // group_rows

    waves = by_offset(wavenumber_of_slot.reshape(count, slots), me)
    chosen = by_offset(lat_order.reshape(count, rows), me)
    chosen = chosen.reshape(count, groups, group_rows).transpose(2, 0, 1).reshape(-1)
    column = lax.broadcasted_iota(jnp.int32, (latitudes, latitudes), 1)
    select = (chosen[:, None] == column).astype(jnp.bfloat16)
    drive = amplitude * jnp.sqrt(1.0 - decay * decay)[:, None]
    drive = jnp.pad(drive, ((0, 8 - scales), (0, 0)))

    old = coeffs_old.transpose(0, 2, 3, 1, 4)
    fresh_noise = noise.transpose(0, 2, 3, 1, 4)
    new = None
    received = []
    start = 0
    pairs = {d: [(a, a ^ d) for a in range(count)] for d in range(1, count)}
    parts = chunks_of(slots)
    for size in parts:
        new, messages = spectral(
            old, fresh_noise, legendre, drive, decay, waves[0], select, start, size, new,
            count, groups, group_rows,
        )
        received.append(
            [messages[0]] + [lax.ppermute(messages[d], AXES, pairs[d]) for d in range(1, count)]
        )
        start += size
    pattern = None
    start = 0
    for index, size in enumerate(parts):
        table = synthesis_table(waves[:, start : start + size], round_up(2 * size, 8), LON)
        final = index == len(parts) - 1
        pattern = synthesis(table, received[index], pattern, final, groups, group_rows, members)
        start += size
    return (new.transpose(0, 3, 1, 2, 4), pattern)


def solution(mesh):
    in_specs = (
        P(AXES, None, None, None, None),
        P(AXES, None, None, None, None),
        P(AXES, None, None),
        P(),
        P(),
        P(),
        P(),
    )
    out_specs = (P(AXES, None, None, None, None), P(AXES, None, None))
    return jax.shard_map(local, mesh=mesh, in_specs=in_specs, out_specs=out_specs, check_vma=False)
```

```python
import jax
import jax.numpy as jnp
from jax import lax
from jax.experimental import pallas as pl
from jax.experimental.layout import Layout, with_layout_constraint
from jax.experimental.pallas import tpu as pltpu
from jax.sharding import PartitionSpec as P

TWO_PI = 6.283185307179586
LON = 1280
LANES = 128
AXES = ("lat", "lon")


def chunks_of(slots):
    if slots % 4:
        return (slots,)
    if slots >= 16:
        return (4, slots - 8, 4)
    return (slots,)


def round_up(value, unit):
    return -(-value // unit) * unit


def dense(values):
    slots, parts, scales, members, width = values.shape
    split = values.reshape(slots, parts, scales, members, width // LANES, LANES)
    split = with_layout_constraint(split, Layout((0, 2, 3, 4, 1, 5)))
    return split.transpose(0, 2, 3, 4, 1, 5).reshape(-1, LANES)


def undense(values, shape):
    slots, parts, scales, members, width = shape
    split = values.reshape(slots, scales, members, width // LANES, parts, LANES)
    return split.transpose(0, 1, 2, 4, 3, 5).reshape(slots, scales, members, parts, width).transpose(
        0, 3, 1, 2, 4
    )


def spectral_kernel(
    first, unit, count, groups, group_rows, members, rows_p, scales, width, base, waves, decay,
    old, noise, legendre, amplitude, select, *rest
):
    new, out, drive, loud, spectrum, rows = rest[0 if first else 1 :]
    step = pl.program_id(0)
    half = spectrum.shape[1] // 4
    blocks = count * groups
    tiles = width // LANES
    stride = 2 * tiles
    per_slot = scales * members * stride

    @pl.when(step == 0)
    def _():
        spectrum[...] = jnp.zeros_like(spectrum)
        if rows_p != 2 * unit * pl.num_programs(0):
            out[...] = jnp.zeros_like(out)
        for k in range(scales):
            d = jnp.full((1, LANES), decay[k], jnp.float32)
            factor = jnp.sqrt(1.0 - d * d)[:, :1]
            drive[k : k + 1] = amplitude[k : k + 1] * factor

    loud[...] = noise[...].astype(jnp.float32)
    lane = lax.broadcasted_iota(jnp.int32, (1, LANES), 1)
    wide_lane = lax.broadcasted_iota(jnp.int32, (blocks, LANES), 1)
    nt = (((1,), (1,)), ((), ()))
    for u in range(unit):
        wave = waves[base[0] + step * unit + u]
        gains = pltpu.roll(drive[...], lax.rem(width - wave, width), 1)
        for tile in range(tiles):
            live = lane + (tile * LANES) + wave < width
            keep = [jnp.where(live, decay[k], 0.0) for k in range(scales)]
            gain = [
                jnp.where(live, gains[k : k + 1, tile * LANES : (tile + 1) * LANES], 0.0)
                for k in range(scales)
            ]
            for r in range(2):
                total = None
                for k in range(scales):
                    at = pl.ds(u * per_slot + k * members * stride + 2 * tile + r, members, stride=stride)
                    fresh = keep[k] * old[at, :] + gain[k] * loud[at, :]
                    new[at, :] = fresh
                    total = fresh if total is None else total + fresh
                high = total.astype(jnp.bfloat16)
                low = (total - high.astype(jnp.float32)).astype(jnp.bfloat16)
                cut = slice(tile * LANES, (tile + 1) * LANES)
                spectrum[u, r * half : r * half + members, cut] = high
                spectrum[u, (2 + r) * half : (2 + r) * half + members, cut] = low
        basis = legendre[u]
        basis_high = basis.astype(jnp.bfloat16)
        basis_low = (basis - basis_high.astype(jnp.float32)).astype(jnp.bfloat16)
        wide = lax.dot_general(basis_high, spectrum[u], nt, preferred_element_type=jnp.float32)
        narrow = lax.dot_general(
            basis_low, spectrum[u, : 2 * half], nt, preferred_element_type=jnp.float32
        )
        field = wide[:, : 2 * half] + wide[:, 2 * half :] + narrow
        field_high = field.astype(jnp.bfloat16)
        field_low = (field - field_high.astype(jnp.float32)).astype(jnp.bfloat16)
        both = jnp.dot(
            select[...],
            jnp.concatenate([field_high, field_low], axis=1),
            preferred_element_type=jnp.float32,
        )
        rows[u] = both[:, : 2 * half] + both[:, 2 * half :]
        for r in range(2):
            packed = [None, None]
            for i in range(group_rows):
                start = i * members
                piece = rows[u, pl.ds(i, blocks, stride=group_rows), :]
                shift = (start - r * half) % LANES
                if shift:
                    piece = pltpu.roll(piece, shift, 1)
                for tile in range(2):
                    begin = max(start - tile * LANES, 0)
                    end = min(start + members - tile * LANES, LANES)
                    if begin >= end:
                        continue
                    if packed[tile] is None:
                        packed[tile] = piece
                    else:
                        packed[tile] = jnp.where(wide_lane < begin, packed[tile], piece)
            for tile in range(2):
                at = pl.ds(tile * rows_p + 2 * (step * unit + u) + r, blocks, stride=2 * rows_p)
                out[at, :] = packed[tile]


def spectral(old, noise, legendre, amplitude, decay, waves, base, select, shape, start, slots, previous, count, groups, group_rows):
    _, _, scales, members, width = shape
    unit = 2 if slots % 2 == 0 else slots
    rows_p = round_up(2 * slots, 8)
    first = previous is None
    size = groups * 2 * rows_p
    block = unit * scales * members * 2 * (width // LANES)
    skip = start // unit

    def body(*refs):
        spectral_kernel(
            first, unit, count, groups, group_rows, members, rows_p, scales, width, *refs
        )

    state = pl.BlockSpec((block, LANES), lambda i: (skip + i, 0))
    in_specs = [
        pl.BlockSpec(memory_space=pltpu.SMEM),
        pl.BlockSpec(memory_space=pltpu.SMEM),
        pl.BlockSpec(memory_space=pltpu.SMEM),
        state,
        state,
        pl.BlockSpec((unit,) + legendre.shape[1:], lambda i: (skip + i, 0, 0)),
        pl.BlockSpec(amplitude.shape, lambda i: (0, 0)),
        pl.BlockSpec(select.shape, lambda i: (0, 0)),
    ]
    args = [base + start, waves, decay, old, noise, legendre, amplitude, select]
    aliases = {}
    if not first:
        in_specs.append(pl.BlockSpec(memory_space=pl.ANY))
        aliases = {len(args): 0}
        args.append(previous)
    new, messages = pl.pallas_call(
        body,
        grid=(slots // unit,),
        in_specs=in_specs,
        out_specs=[state, pl.BlockSpec((count * size, LANES), lambda i: (0, 0))],
        out_shape=[
            jax.ShapeDtypeStruct(old.shape, jnp.float32),
            jax.ShapeDtypeStruct((count * size, LANES), jnp.float32),
        ],
        scratch_shapes=[
            pltpu.VMEM((8, width), jnp.float32),
            pltpu.VMEM((block, LANES), jnp.float32),
            pltpu.VMEM((unit, 4 * 64, width), jnp.bfloat16),
            pltpu.VMEM((unit, legendre.shape[1], LANES), jnp.float32),
        ],
        input_output_aliases=aliases,
        compiler_params=pltpu.CompilerParams(dimension_semantics=("arbitrary",)),
        cost_estimate=pl.CostEstimate(
            flops=slots * 2 * 10**9 // 4, bytes_accessed=slots * 3500000, transcendentals=0
        ),
        name="spectral",
    )(*args)
    return new, messages.reshape(count, size, LANES)


def synthesis_kernel(has_previous, final, count, rows_p, members, group_rows, fine, coarse, sources, *rest):
    previous = None
    if has_previous:
        previous = rest[0]
        rest = rest[1:]
    out, table_high, table_low, stack = rest
    group = pl.program_id(0)
    length = table_high.shape[1]

    @pl.when(group == 0)
    def _():
        even = fine[0]
        odd = fine[1]
        for b in range(length // LANES):
            values = even * coarse[0, :, b : b + 1] - odd * coarse[1, :, b : b + 1]
            high = values.astype(jnp.bfloat16)
            cut = slice(b * LANES, (b + 1) * LANES)
            table_high[:, cut] = high
            table_low[:, cut] = (values - high.astype(jnp.float32)).astype(jnp.bfloat16)

    for d in range(count):
        for tile in range(2):
            offset = pl.multiple_of((group * 2 + tile) * rows_p, 8)
            stack[d * rows_p : (d + 1) * rows_p, tile * LANES : (tile + 1) * LANES] = sources[
                d, pl.ds(offset, rows_p), :
            ]
    turned = stack[...].T
    high = turned.astype(jnp.bfloat16)
    low = (turned - high.astype(jnp.float32)).astype(jnp.bfloat16)
    result = jnp.dot(high, table_high[...], preferred_element_type=jnp.float32)
    result += jnp.dot(low, table_high[...], preferred_element_type=jnp.float32)
    result += jnp.dot(high, table_low[...], preferred_element_type=jnp.float32)
    if has_previous:
        result += previous[0]
    if final:
        for i in range(group_rows):
            out[i] = result[i * members : (i + 1) * members]
    else:
        out[0] = result


def synthesis(fine, coarse, sources, previous, final, groups, group_rows, members, length):
    count = sources.shape[0]
    depth = fine.shape[1]
    rows_p = depth // count

    def body(*refs):
        synthesis_kernel(previous is not None, final, count, rows_p, members, group_rows, *refs)

    in_specs = [
        pl.BlockSpec(fine.shape, lambda g: (0, 0, 0)),
        pl.BlockSpec(coarse.shape, lambda g: (0, 0, 0)),
        pl.BlockSpec(sources.shape, lambda g: (0, 0, 0)),
    ]
    args = [fine, coarse, sources]
    partial = pl.BlockSpec((1, 2 * LANES, length), lambda g: (g, 0, 0))
    aliases = {}
    if previous is not None:
        in_specs.append(partial)
        if not final:
            aliases = {len(args): 0}
        args.append(previous)
    if final:
        out_spec = pl.BlockSpec((group_rows, members, length), lambda g: (g, 0, 0))
        out_shape = jax.ShapeDtypeStruct((groups * group_rows, members, length), jnp.float32)
    else:
        out_spec = partial
        out_shape = jax.ShapeDtypeStruct((groups, 2 * LANES, length), jnp.float32)
    return pl.pallas_call(
        body,
        grid=(groups,),
        in_specs=in_specs,
        out_specs=out_spec,
        out_shape=out_shape,
        scratch_shapes=[
            pltpu.VMEM((depth, length), jnp.bfloat16),
            pltpu.VMEM((depth, length), jnp.bfloat16),
            pltpu.VMEM((depth, 2 * LANES), jnp.float32),
        ],
        input_output_aliases=aliases,
        compiler_params=pltpu.CompilerParams(dimension_semantics=("arbitrary",)),
        cost_estimate=pl.CostEstimate(
            flops=6 * groups * 256 * depth * length, bytes_accessed=12 * 10**6, transcendentals=0
        ),
        name="synthesis",
    )(*args)


def synthesis_tables(waves, parts, length):
    count, slots = waves.shape
    numbers = []
    start = 0
    for size in parts:
        rows = jnp.repeat(waves[:, start : start + size], 2, axis=1)
        pad = round_up(2 * size, 8) - 2 * size
        numbers.append(jnp.pad(rows, ((0, 0), (0, pad)), constant_values=-1).reshape(-1))
        start += size
    number = jnp.concatenate(numbers)[:, None]
    lane = lax.broadcasted_iota(jnp.int32, (number.shape[0], LANES), 1)
    part = lax.broadcasted_iota(jnp.int32, (number.shape[0], LANES), 0) % 2
    weight = jnp.where(number == 0, 1.0, jnp.where(number < 0, 0.0, 2.0)).astype(jnp.float32)
    wave = jnp.maximum(number, 0)
    near = ((wave * lane + part * (length // 4)) % length).astype(jnp.float32) * (TWO_PI / length)
    far = ((wave * (lane * LANES % length)) % length).astype(jnp.float32) * (TWO_PI / length)
    fine = jnp.stack([weight * jnp.cos(near), weight * jnp.sin(near)])
    coarse = jnp.stack([jnp.cos(far), jnp.sin(far)])
    return fine, coarse


def local(coeffs_old, noise, legendre, decay, amplitude, wavenumber_of_slot, lat_order):
    lat_count = lax.axis_size("lat")
    lon_count = lax.axis_size("lon")
    count = lat_count * lon_count
    me = lax.axis_index("lat") * lon_count + lax.axis_index("lon")
    shape = coeffs_old.shape
    slots, _, scales, members, width = shape
    latitudes = lat_order.shape[0]
    rows = latitudes // count
    group_rows = (2 * LANES) // members
    while rows % group_rows:
        group_rows -= 1
    groups = rows // group_rows

    column = lax.broadcasted_iota(jnp.int32, (latitudes, latitudes), 1)
    select = (lat_order[:, None] == column).astype(jnp.bfloat16)
    base = (me * slots).reshape(1).astype(jnp.int32)

    old = dense(coeffs_old)
    fresh_noise = dense(noise)
    parts = chunks_of(slots)
    new = None
    received = []
    start = 0
    waves = wavenumber_of_slot
    for size in parts:
        new, messages = spectral(
            old, fresh_noise, legendre, amplitude, decay, wavenumber_of_slot, base, select, shape,
            start, size, new, count, groups, group_rows,
        )
        if start == 0:
            messages, waves = lax.optimization_barrier((messages, waves))
        received.append(lax.all_to_all(messages, AXES, 0, 0, tiled=True))
        start += size
    fine, coarse = synthesis_tables(waves.reshape(count, slots), parts, LON)
    pattern = None
    start = 0
    for index, size in enumerate(parts):
        depth = count * round_up(2 * size, 8)
        pattern = synthesis(
            fine[:, start : start + depth], coarse[:, start : start + depth], received[index],
            pattern, index == len(parts) - 1, groups, group_rows, members, LON,
        )
        start += depth
    return (undense(new, shape), pattern)


def solution(mesh):
    in_specs = (
        P(AXES, None, None, None, None),
        P(AXES, None, None, None, None),
        P(AXES, None, None),
        P(),
        P(),
        P(),
        P(),
    )
    out_specs = (P(AXES, None, None, None, None), P(AXES, None, None))
    return jax.shard_map(local, mesh=mesh, in_specs=in_specs, out_specs=out_specs, check_vma=False)
```

```python
import jax
import jax.numpy as jnp
from jax import lax
from jax.experimental import pallas as pl
from jax.experimental.layout import Layout, with_layout_constraint
from jax.experimental.pallas import tpu as pltpu
from jax.sharding import PartitionSpec as P

TWO_PI = 6.283185307179586
LON = 1280
LANES = 128
AXES = ("lat", "lon")


def chunks_of(slots):
    if slots % 4:
        return (slots,)
    if slots >= 16:
        return (4, slots - 8, 4)
    return (slots,)


def round_up(value, unit):
    return -(-value // unit) * unit


def dense(values):
    slots, parts, scales, members, width = values.shape
    split = values.reshape(slots, parts, scales, members, width // LANES, LANES)
    split = with_layout_constraint(split, Layout((0, 2, 3, 4, 1, 5)))
    return split.transpose(0, 2, 3, 4, 1, 5).reshape(-1, LANES)


def undense(values, shape):
    slots, parts, scales, members, width = shape
    split = values.reshape(slots, scales, members, width // LANES, parts, LANES)
    return split.transpose(0, 1, 2, 4, 3, 5).reshape(slots, scales, members, parts, width).transpose(
        0, 3, 1, 2, 4
    )


def spectral_kernel(
    first, slots, unit, count, groups, group_rows, members, rows_p, scales, width, base, waves,
    decay, old, noise, legendre, amplitude, order, *rest
):
    new, out, drive, loud, spectrum, rows, select = rest[0 if first else 1 :]
    step = pl.program_id(0)
    half = spectrum.shape[1] // 4
    blocks = count * groups
    tiles = width // LANES
    stride = 2 * tiles
    per_slot = scales * members * stride

    @pl.when(step == 0)
    def _():
        spectrum[...] = jnp.zeros_like(spectrum)
        if rows_p != 2 * slots:
            out[...] = jnp.zeros_like(out)
        for k in range(scales):
            d = jnp.full((1, LANES), decay[k], jnp.float32)
            factor = jnp.sqrt(1.0 - d * d)[:, :1]
            drive[k : k + 1] = amplitude[k : k + 1] * factor
        lines = order.shape[0]
        listed = order[...].astype(jnp.float32)
        padding = jnp.zeros((round_up(lines, 8) - lines, LANES), jnp.float32)
        listed = jnp.concatenate([listed, padding], axis=0).T
        latitude = lax.broadcasted_iota(jnp.int32, (LANES, select.shape[1]), 1).astype(jnp.float32)
        for b in range(lines):
            hit = jnp.where(listed[:, b : b + 1] == latitude, 1.0, 0.0)
            select[b * LANES : (b + 1) * LANES] = hit.astype(jnp.bfloat16)

    loud[...] = noise[...].astype(jnp.float32)
    lane = lax.broadcasted_iota(jnp.int32, (1, LANES), 1)
    wide_lane = lax.broadcasted_iota(jnp.int32, (blocks, LANES), 1)
    nt = (((1,), (1,)), ((), ()))
    for u in range(unit):
        wave = waves[base[0] + step * unit + u]
        gains = pltpu.roll(drive[...], lax.rem(width - wave, width), 1)
        for tile in range(tiles):
            live = lane + (tile * LANES) + wave < width
            keep = [jnp.where(live, decay[k], 0.0) for k in range(scales)]
            gain = [
                jnp.where(live, gains[k : k + 1, tile * LANES : (tile + 1) * LANES], 0.0)
                for k in range(scales)
            ]
            for r in range(2):
                total = None
                for k in range(scales):
                    at = pl.ds(u * per_slot + k * members * stride + 2 * tile + r, members, stride=stride)
                    fresh = keep[k] * old[at, :] + gain[k] * loud[at, :]
                    new[at, :] = fresh
                    total = fresh if total is None else total + fresh
                high = total.astype(jnp.bfloat16)
                low = (total - high.astype(jnp.float32)).astype(jnp.bfloat16)
                cut = slice(tile * LANES, (tile + 1) * LANES)
                spectrum[u, r * half : r * half + members, cut] = high
                spectrum[u, (2 + r) * half : (2 + r) * half + members, cut] = low
        basis = legendre[u]
        basis_high = basis.astype(jnp.bfloat16)
        basis_low = (basis - basis_high.astype(jnp.float32)).astype(jnp.bfloat16)
        wide = lax.dot_general(basis_high, spectrum[u], nt, preferred_element_type=jnp.float32)
        narrow = lax.dot_general(
            basis_low, spectrum[u, : 2 * half], nt, preferred_element_type=jnp.float32
        )
        field = wide[:, : 2 * half] + wide[:, 2 * half :] + narrow
        field_high = field.astype(jnp.bfloat16)
        field_low = (field - field_high.astype(jnp.float32)).astype(jnp.bfloat16)
        both = jnp.dot(
            select[...],
            jnp.concatenate([field_high, field_low], axis=1),
            preferred_element_type=jnp.float32,
        )
        rows[u] = both[:, : 2 * half] + both[:, 2 * half :]
        for r in range(2):
            packed = [None, None]
            for i in range(group_rows):
                start = i * members
                piece = rows[u, pl.ds(i, blocks, stride=group_rows), :]
                shift = (start - r * half) % LANES
                if shift:
                    piece = pltpu.roll(piece, shift, 1)
                for tile in range(2):
                    begin = max(start - tile * LANES, 0)
                    end = min(start + members - tile * LANES, LANES)
                    if begin >= end:
                        continue
                    if packed[tile] is None:
                        packed[tile] = piece
                    else:
                        packed[tile] = jnp.where(wide_lane < begin, packed[tile], piece)
            for tile in range(2):
                at = pl.ds(tile * rows_p + 2 * (step * unit + u) + r, blocks, stride=2 * rows_p)
                out[at, :] = packed[tile]


def spectral(old, noise, legendre, amplitude, decay, waves, base, order, shape, start, slots, previous, count, groups, group_rows):
    _, _, scales, members, width = shape
    unit = 2 if slots % 2 == 0 else slots
    rows_p = round_up(2 * slots, 8)
    first = previous is None
    size = groups * 2 * rows_p
    block = unit * scales * members * 2 * (width // LANES)
    skip = start // unit

    def body(*refs):
        spectral_kernel(
            first, slots, unit, count, groups, group_rows, members, rows_p, scales, width, *refs
        )

    state = pl.BlockSpec((block, LANES), lambda i: (skip + i, 0))
    in_specs = [
        pl.BlockSpec(memory_space=pltpu.SMEM),
        pl.BlockSpec(memory_space=pltpu.SMEM),
        pl.BlockSpec(memory_space=pltpu.SMEM),
        state,
        state,
        pl.BlockSpec((unit,) + legendre.shape[1:], lambda i: (skip + i, 0, 0)),
        pl.BlockSpec(amplitude.shape, lambda i: (0, 0)),
        pl.BlockSpec(order.shape, lambda i: (0, 0)),
    ]
    args = [base + start, waves, decay, old, noise, legendre, amplitude, order]
    aliases = {}
    if not first:
        in_specs.append(pl.BlockSpec(memory_space=pl.ANY))
        aliases = {len(args): 0}
        args.append(previous)
    new, messages = pl.pallas_call(
        body,
        grid=(slots // unit,),
        in_specs=in_specs,
        out_specs=[state, pl.BlockSpec((count * size, LANES), lambda i: (0, 0))],
        out_shape=[
            jax.ShapeDtypeStruct(old.shape, jnp.float32),
            jax.ShapeDtypeStruct((count * size, LANES), jnp.float32),
        ],
        scratch_shapes=[
            pltpu.VMEM((8, width), jnp.float32),
            pltpu.VMEM((block, LANES), jnp.float32),
            pltpu.VMEM((unit, 4 * 64, width), jnp.bfloat16),
            pltpu.VMEM((unit, legendre.shape[1], LANES), jnp.float32),
            pltpu.VMEM((legendre.shape[1], legendre.shape[1]), jnp.bfloat16),
        ],
        input_output_aliases=aliases,
        compiler_params=pltpu.CompilerParams(
            dimension_semantics=("arbitrary",), vmem_limit_bytes=65400 * 2**10
        ),
        cost_estimate=pl.CostEstimate(
            flops=slots * 2 * 10**9 // 4, bytes_accessed=slots * 3500000, transcendentals=0
        ),
        name="spectral",
    )(*args)
    return new, messages.reshape(count, size, LANES)


def table_kernel(fine, coarse, high, low):
    even = fine[0]
    odd = fine[1]
    for b in range(high.shape[1] // LANES):
        values = even * coarse[0, :, b : b + 1] - odd * coarse[1, :, b : b + 1]
        rounded = values.astype(jnp.bfloat16)
        cut = slice(b * LANES, (b + 1) * LANES)
        high[:, cut] = rounded
        low[:, cut] = (values - rounded.astype(jnp.float32)).astype(jnp.bfloat16)


def expand_tables(fine, coarse, start, depth, length):
    rows = 256 if start % 256 == 0 and depth % 256 == 0 else depth
    factor = pl.BlockSpec((2, rows, LANES), lambda i: (0, start // rows + i, 0))
    table = pl.BlockSpec((rows, length), lambda i: (i, 0))
    return pl.pallas_call(
        table_kernel,
        grid=(depth // rows,),
        in_specs=[factor, factor],
        out_specs=[table, table],
        out_shape=[jax.ShapeDtypeStruct((depth, length), jnp.bfloat16)] * 2,
        compiler_params=pltpu.CompilerParams(
            dimension_semantics=("arbitrary",), vmem_limit_bytes=16 * 2**20
        ),
        cost_estimate=pl.CostEstimate(
            flops=2 * 10**9 * depth // 1024, bytes_accessed=depth * length * 4, transcendentals=0
        ),
        name="tables",
    )(fine, coarse)


def synthesis_kernel(has_previous, final, groups, group_rows, members, table_high, table_low, sources, *rest):
    previous = None
    if has_previous:
        previous = rest[0]
        rest = rest[1:]
    (out,) = rest
    count = sources.shape[0]
    depth = table_high.shape[0]
    rows_p = depth // count

    pieces = []
    for tile in range(2):
        pieces.append(sources[:, tile * rows_p : (tile + 1) * rows_p, :].reshape(depth, LANES).T)
    piece = jnp.concatenate(pieces, axis=0)
    high = piece.astype(jnp.bfloat16)
    low = (piece - high.astype(jnp.float32)).astype(jnp.bfloat16)
    result = jnp.dot(high, table_high[...], preferred_element_type=jnp.float32)
    result += jnp.dot(low, table_high[...], preferred_element_type=jnp.float32)
    result += jnp.dot(high, table_low[...], preferred_element_type=jnp.float32)
    if has_previous:
        result += previous[...]
    if final:
        for i in range(group_rows):
            out[i] = result[i * members : (i + 1) * members]
    else:
        out[...] = result


def synthesis(tables, sources, previous, final, groups, group_rows, members):
    depth, length = tables[0].shape

    def body(*refs):
        synthesis_kernel(previous is not None, final, groups, group_rows, members, *refs)

    rows_p = depth // sources.shape[0]
    table = pl.BlockSpec((depth, length), lambda b: (0, 0))
    partial = pl.BlockSpec((2 * LANES, length), lambda b: (b, 0))
    in_specs = [table, table, pl.BlockSpec((sources.shape[0], 2 * rows_p, LANES), lambda b: (0, b, 0))]
    space = pltpu.VMEM if final else pltpu.HBM
    args = [pltpu.with_memory_space_constraint(table_part, pltpu.HBM) for table_part in tables]
    args.append(pltpu.with_memory_space_constraint(sources, space))
    if previous is not None:
        in_specs.append(partial)
        args.append(pltpu.with_memory_space_constraint(previous, pltpu.HBM))
    if final:
        out_spec = pl.BlockSpec((group_rows, members, length), lambda b: (b, 0, 0))
        out_shape = jax.ShapeDtypeStruct((groups * group_rows, members, length), jnp.float32)
    else:
        out_spec = partial
        out_shape = pltpu.HBM((groups * 2 * LANES, length), jnp.float32)
    return pl.pallas_call(
        body,
        grid=(groups,),
        in_specs=in_specs,
        out_specs=out_spec,
        out_shape=out_shape,
        compiler_params=pltpu.CompilerParams(
            dimension_semantics=("arbitrary",), vmem_limit_bytes=26 * 2**20
        ),
        cost_estimate=pl.CostEstimate(
            flops=6 * groups * 256 * depth * length, bytes_accessed=12 * 10**6, transcendentals=0
        ),
        name="synthesis",
    )(*args)


def synthesis_tables(waves, parts, length):
    count, slots = waves.shape
    numbers = []
    start = 0
    for size in parts:
        rows = jnp.repeat(waves[:, start : start + size], 2, axis=1)
        pad = round_up(2 * size, 8) - 2 * size
        numbers.append(jnp.pad(rows, ((0, 0), (0, pad)), constant_values=-1).reshape(-1))
        start += size
    number = jnp.concatenate(numbers)[:, None]
    lane = lax.broadcasted_iota(jnp.int32, (number.shape[0], LANES), 1)
    part = lax.broadcasted_iota(jnp.int32, (number.shape[0], LANES), 0) % 2
    weight = jnp.where(number == 0, 1.0, jnp.where(number < 0, 0.0, 2.0)).astype(jnp.float32)
    wave = jnp.maximum(number, 0)
    near = ((wave * lane + part * (length // 4)) % length).astype(jnp.float32) * (TWO_PI / length)
    far = ((wave * (lane * LANES % length)) % length).astype(jnp.float32) * (TWO_PI / length)
    fine = jnp.stack([weight * jnp.cos(near), weight * jnp.sin(near)])
    coarse = jnp.stack([jnp.cos(far), jnp.sin(far)])
    return fine, coarse


def local(coeffs_old, noise, legendre, decay, amplitude, wavenumber_of_slot, lat_order):
    lat_count = lax.axis_size("lat")
    lon_count = lax.axis_size("lon")
    count = lat_count * lon_count
    me = lax.axis_index("lat") * lon_count + lax.axis_index("lon")
    shape = coeffs_old.shape
    slots, _, scales, members, width = shape
    latitudes = lat_order.shape[0]
    rows = latitudes // count
    group_rows = (2 * LANES) // members
    while rows % group_rows:
        group_rows -= 1
    groups = rows // group_rows

    order = lat_order.reshape(-1, LANES)
    base = (me * slots).reshape(1).astype(jnp.int32)

    old = dense(coeffs_old)
    fresh_noise = dense(noise)
    parts = chunks_of(slots)
    last = len(parts) - 1
    starts = [sum(parts[:i]) for i in range(len(parts))]
    depths = [count * round_up(2 * size, 8) for size in parts]
    new = None
    pattern = None
    received = []
    tables = []
    for index, size in enumerate(parts):
        new, messages = spectral(
            old, fresh_noise, legendre, amplitude, decay, wavenumber_of_slot, base, order, shape,
            starts[index], size, new, count, groups, group_rows,
        )
        if index == 0:
            messages, waves = lax.optimization_barrier((messages, wavenumber_of_slot))
            fine, coarse = synthesis_tables(waves.reshape(count, slots), parts, LON)
            tables = [
                expand_tables(fine, coarse, sum(depths[:i]), depths[i], LON) for i in range(len(parts))
            ]
        if index == 2:
            pattern = synthesis(
                tables[0], received[0], None, False, groups, group_rows, members
            )
        if index == last and index:
            messages, pattern, tables = lax.optimization_barrier((messages, pattern, tables))
        received.append(lax.all_to_all(messages, AXES, 0, 0, tiled=True))
    for index in range(1 if last >= 2 else 0, len(parts)):
        pattern = synthesis(
            tables[index], received[index], pattern, index == last,
            groups, group_rows, members,
        )
    return (undense(new, shape), pattern)


def solution(mesh):
    in_specs = (
        P(AXES, None, None, None, None),
        P(AXES, None, None, None, None),
        P(AXES, None, None),
        P(),
        P(),
        P(),
        P(),
    )
    out_specs = (P(AXES, None, None, None, None), P(AXES, None, None))
    return jax.shard_map(local, mesh=mesh, in_specs=in_specs, out_specs=out_specs, check_vma=False)
```

```python
import jax
import jax.numpy as jnp
from jax import lax
from jax.experimental import pallas as pl
from jax.experimental.layout import Layout, with_layout_constraint
from jax.experimental.pallas import tpu as pltpu
from jax.sharding import PartitionSpec as P

TWO_PI = 6.283185307179586
LON = 1280
LANES = 128
AXES = ("lat", "lon")


def chunks_of(slots):
    if slots % 4 or slots < 16:
        return ((0, slots),)
    return ((slots - 4, 4), (0, slots - 8), (slots - 8, 4))


def round_up(value, unit):
    return -(-value // unit) * unit


def dense(values):
    slots, parts, scales, members, width = values.shape
    split = values.reshape(slots, parts, scales, members, width // LANES, LANES)
    split = with_layout_constraint(split, Layout((0, 2, 3, 4, 1, 5)))
    return split.transpose(0, 2, 3, 4, 1, 5).reshape(-1, LANES)


def undense(values, shape):
    slots, parts, scales, members, width = shape
    split = values.reshape(slots, scales, members, width // LANES, parts, LANES)
    return split.transpose(0, 1, 2, 4, 3, 5).reshape(slots, scales, members, parts, width).transpose(
        0, 3, 1, 2, 4
    )


def spectral_kernel(
    fill, first, start, slots, unit, count, groups, group_rows, members, rows_p, scales, width, base, waves,
    decay, old, noise, legendre, amplitude, order, *rest
):
    rest = rest[0 if first else 1 :]
    new = rest[0] if fill else None
    out, drive, loud, spectrum, rows, select, bases, sems = rest[1 if fill else 0 :]
    step = pl.program_id(0)
    half = spectrum.shape[1] // 4
    blocks = count * groups
    tiles = width // LANES
    stride = 2 * tiles
    per_slot = scales * members * stride

    @pl.when(step == 0)
    def _():
        spectrum[...] = jnp.zeros_like(spectrum)
        if rows_p != 2 * slots:
            out[...] = jnp.zeros_like(out)
        for k in range(scales):
            d = jnp.full((1, LANES), decay[k], jnp.float32)
            factor = jnp.sqrt(1.0 - d * d)[:, :1]
            drive[k : k + 1] = amplitude[k : k + 1] * factor
        lines = order.shape[0]
        listed = order[...].astype(jnp.float32)
        padding = jnp.zeros((round_up(lines, 8) - lines, LANES), jnp.float32)
        listed = jnp.concatenate([listed, padding], axis=0).T
        latitude = lax.broadcasted_iota(jnp.int32, (LANES, select.shape[1]), 1).astype(jnp.float32)
        for b in range(lines):
            hit = jnp.where(listed[:, b : b + 1] == latitude, 1.0, 0.0)
            select[b * LANES : (b + 1) * LANES] = hit.astype(jnp.bfloat16)

    loud[...] = noise[...].astype(jnp.float32)
    lane = lax.broadcasted_iota(jnp.int32, (1, LANES), 1)
    wide_lane = lax.broadcasted_iota(jnp.int32, (blocks, LANES), 1)
    nt = (((1,), (1,)), ((), ()))
    steps = slots // unit
    levels = sorted({max(1, 2 * tiles // 5), tiles})
    buffer = lax.rem(step, 2)

    def is_level(index, level):
        lowest = waves[base[0] + index * unit]
        for u in range(1, unit):
            lowest = jnp.minimum(lowest, waves[base[0] + index * unit + u])
        few = lowest + levels[0] * LANES >= width
        return few if level != tiles else jnp.logical_not(few)

    def copies(index, level):
        reach = pl.ds(0, level * LANES)
        into = lax.rem(index, 2)
        return [
            pltpu.make_async_copy(
                legendre.at[start + index * unit + u, :, reach],
                bases.at[into, u, :, reach],
                sems.at[into, u],
            )
            for u in range(unit)
        ]

    def begin_copies(index):
        for level in levels:

            @pl.when(is_level(index, level))
            def _():
                for copy in copies(index, level):
                    copy.start()

    @pl.when(step == 0)
    def _():
        begin_copies(0)

    @pl.when(step + 1 < steps)
    def _():
        begin_copies(step + 1)

    def work(level):
        for copy in copies(step, level):
            copy.wait()
        for u in range(unit):
            wave = waves[base[0] + step * unit + u]
            gains = pltpu.roll(drive[...], lax.rem(width - wave, width), 1)
            for tile in range(level if fill else tiles, tiles):
                for r in range(2):
                    for k in range(scales):
                        at = pl.ds(u * per_slot + k * members * stride + 2 * tile + r, members, stride=stride)
                        new[at, :] = jnp.zeros((members, LANES), jnp.float32)
            for tile in range(level):
                live = lane + (tile * LANES) + wave < width
                keep = [jnp.where(live, decay[k], 0.0) for k in range(scales)]
                gain = [
                    jnp.where(live, gains[k : k + 1, tile * LANES : (tile + 1) * LANES], 0.0)
                    for k in range(scales)
                ]
                for r in range(2):
                    total = None
                    for k in range(scales):
                        at = pl.ds(u * per_slot + k * members * stride + 2 * tile + r, members, stride=stride)
                        fresh = keep[k] * old[at, :] + gain[k] * loud[at, :]
                        if fill:
                            new[at, :] = fresh
                        total = fresh if total is None else total + fresh
                    high = total.astype(jnp.bfloat16)
                    low = (total - high.astype(jnp.float32)).astype(jnp.bfloat16)
                    cut = slice(tile * LANES, (tile + 1) * LANES)
                    spectrum[u, r * half : r * half + members, cut] = high
                    spectrum[u, (2 + r) * half : (2 + r) * half + members, cut] = low
            reach = level * LANES
            basis = bases[buffer, u, :, :reach]
            basis_high = basis.astype(jnp.bfloat16)
            basis_low = (basis - basis_high.astype(jnp.float32)).astype(jnp.bfloat16)
            wide = lax.dot_general(basis_high, spectrum[u, :, :reach], nt, preferred_element_type=jnp.float32)
            narrow = lax.dot_general(
                basis_low, spectrum[u, : 2 * half, :reach], nt, preferred_element_type=jnp.float32
            )
            field = wide[:, : 2 * half] + wide[:, 2 * half :] + narrow
            field_high = field.astype(jnp.bfloat16)
            field_low = (field - field_high.astype(jnp.float32)).astype(jnp.bfloat16)
            both = jnp.dot(
                select[...],
                jnp.concatenate([field_high, field_low], axis=1),
                preferred_element_type=jnp.float32,
            )
            rows[u] = both[:, : 2 * half] + both[:, 2 * half :]
            for r in range(2):
                packed = [None, None]
                for i in range(group_rows):
                    start = i * members
                    piece = rows[u, pl.ds(i, blocks, stride=group_rows), :]
                    shift = (start - r * half) % LANES
                    if shift:
                        piece = pltpu.roll(piece, shift, 1)
                    for tile in range(2):
                        begin = max(start - tile * LANES, 0)
                        end = min(start + members - tile * LANES, LANES)
                        if begin >= end:
                            continue
                        if packed[tile] is None:
                            packed[tile] = piece
                        else:
                            packed[tile] = jnp.where(wide_lane < begin, packed[tile], piece)
                for tile in range(2):
                    at = pl.ds(tile * rows_p + 2 * (step * unit + u) + r, blocks, stride=2 * rows_p)
                    out[at, :] = packed[tile]

    for level in levels:

        @pl.when(is_level(step, level))
        def _():
            work(level)


def spectral(old, noise, legendre, amplitude, decay, waves, base, order, shape, start, slots, fill, previous, count, groups, group_rows):
    _, _, scales, members, width = shape
    unit = 2 if slots % 2 == 0 else slots
    rows_p = round_up(2 * slots, 8)
    first = previous is None
    size = groups * 2 * rows_p
    block = unit * scales * members * 2 * (width // LANES)
    skip = start // unit

    def body(*refs):
        spectral_kernel(
            fill, first, start, slots, unit, count, groups, group_rows, members, rows_p, scales, width, *refs
        )

    state = pl.BlockSpec((block, LANES), lambda i: (skip + i, 0))
    in_specs = [
        pl.BlockSpec(memory_space=pltpu.SMEM),
        pl.BlockSpec(memory_space=pltpu.SMEM),
        pl.BlockSpec(memory_space=pltpu.SMEM),
        state,
        state,
        pl.BlockSpec(memory_space=pl.ANY),
        pl.BlockSpec(amplitude.shape, lambda i: (0, 0)),
        pl.BlockSpec(order.shape, lambda i: (0, 0)),
    ]
    args = [base + start, waves, decay, old, noise, legendre, amplitude, order]
    aliases = {}
    if not first:
        in_specs.append(pl.BlockSpec(memory_space=pl.ANY))
        aliases = {len(args): 0}
        args.append(previous)
    results = pl.pallas_call(
        body,
        grid=(slots // unit,),
        in_specs=in_specs,
        out_specs=[state] * fill + [pl.BlockSpec((count * size, LANES), lambda i: (0, 0))],
        out_shape=[jax.ShapeDtypeStruct(old.shape, jnp.float32)] * fill
        + [jax.ShapeDtypeStruct((count * size, LANES), jnp.float32)],
        scratch_shapes=[
            pltpu.VMEM((8, width), jnp.float32),
            pltpu.VMEM((block, LANES), jnp.float32),
            pltpu.VMEM((unit, 4 * 64, width), jnp.bfloat16),
            pltpu.VMEM((unit, legendre.shape[1], LANES), jnp.float32),
            pltpu.VMEM((legendre.shape[1], legendre.shape[1]), jnp.bfloat16),
            pltpu.VMEM((2, unit) + legendre.shape[1:], jnp.float32),
            pltpu.SemaphoreType.DMA((2, unit)),
        ],
        input_output_aliases=aliases,
        compiler_params=pltpu.CompilerParams(
            dimension_semantics=("arbitrary",), vmem_limit_bytes=65400 * 2**10
        ),
        cost_estimate=pl.CostEstimate(
            flops=slots * 2 * 10**9 // 4, bytes_accessed=slots * 3500000, transcendentals=0
        ),
        name="spectral",
    )(*args)
    return results[0] if fill else None, results[-1].reshape(count, size, LANES)


def update_kernel(start, unit, members, scales, width, base, waves, decay, old, noise, amplitude, _, new, drive, loud):
    tiles = width // LANES
    stride = 2 * tiles
    for k in range(scales):
        d = jnp.full((1, LANES), decay[k], jnp.float32)
        drive[k : k + 1] = amplitude[k : k + 1] * jnp.sqrt(1.0 - d * d)[:, :1]
    loud[...] = noise[...].astype(jnp.float32)
    lane = lax.broadcasted_iota(jnp.int32, (1, LANES), 1)
    for u in range(unit):
        wave = waves[base[0] + pl.program_id(0) * unit + u]
        gains = pltpu.roll(drive[...], lax.rem(width - wave, width), 1)
        for tile in range(tiles):
            live = lane + (tile * LANES) + wave < width
            for k in range(scales):
                keep = jnp.where(live, decay[k], 0.0)
                gain = jnp.where(live, gains[k : k + 1, tile * LANES : (tile + 1) * LANES], 0.0)
                for r in range(2):
                    row = (u * scales + k) * members * stride + 2 * tile + r
                    at = pl.ds(row, members, stride=stride)
                    new[at, :] = keep * old[at, :] + gain * loud[at, :]


def update(old, noise, amplitude, decay, waves, base, shape, start, slots, previous):
    _, _, scales, members, width = shape
    unit = 2
    block = unit * scales * members * 2 * (width // LANES)
    skip = start // unit

    def body(*refs):
        update_kernel(start, unit, members, scales, width, *refs)

    state = pl.BlockSpec((block, LANES), lambda i: (skip + i, 0))
    return pl.pallas_call(
        body,
        grid=(slots // unit,),
        in_specs=[
            pl.BlockSpec(memory_space=pltpu.SMEM),
            pl.BlockSpec(memory_space=pltpu.SMEM),
            pl.BlockSpec(memory_space=pltpu.SMEM),
            state,
            state,
            pl.BlockSpec(amplitude.shape, lambda i: (0, 0)),
            pl.BlockSpec(memory_space=pl.ANY),
        ],
        out_specs=state,
        out_shape=jax.ShapeDtypeStruct(old.shape, jnp.float32),
        scratch_shapes=[
            pltpu.VMEM((8, width), jnp.float32),
            pltpu.VMEM((block, LANES), jnp.float32),
        ],
        input_output_aliases={6: 0},
        compiler_params=pltpu.CompilerParams(
            dimension_semantics=("arbitrary",), vmem_limit_bytes=65400 * 2**10
        ),
        cost_estimate=pl.CostEstimate(
            flops=slots * 10**8, bytes_accessed=slots * 1900000, transcendentals=0
        ),
        name="update",
    )(base + start, waves, decay, old, noise, amplitude, previous)


def table_kernel(fine, coarse, high, low):
    even = fine[0]
    odd = fine[1]
    for b in range(high.shape[1] // LANES):
        values = even * coarse[0, :, b : b + 1] - odd * coarse[1, :, b : b + 1]
        rounded = values.astype(jnp.bfloat16)
        cut = slice(b * LANES, (b + 1) * LANES)
        high[:, cut] = rounded
        low[:, cut] = (values - rounded.astype(jnp.float32)).astype(jnp.bfloat16)


def expand_tables(fine, coarse, start, depth, length):
    rows = 256 if start % 256 == 0 and depth % 256 == 0 else depth
    factor = pl.BlockSpec((2, rows, LANES), lambda i: (0, start // rows + i, 0))
    table = pl.BlockSpec((rows, length), lambda i: (i, 0))
    return pl.pallas_call(
        table_kernel,
        grid=(depth // rows,),
        in_specs=[factor, factor],
        out_specs=[table, table],
        out_shape=[jax.ShapeDtypeStruct((depth, length), jnp.bfloat16)] * 2,
        compiler_params=pltpu.CompilerParams(
            dimension_semantics=("arbitrary",), vmem_limit_bytes=16 * 2**20
        ),
        cost_estimate=pl.CostEstimate(
            flops=2 * 10**9 * depth // 1024, bytes_accessed=depth * length * 4, transcendentals=0
        ),
        name="tables",
    )(fine, coarse)


def synthesis_kernel(has_previous, final, groups, group_rows, members, table_high, table_low, sources, *rest):
    previous = None
    if has_previous:
        previous = rest[0]
        rest = rest[1:]
    (out,) = rest
    count = sources.shape[0]
    depth = table_high.shape[0]
    rows_p = depth // count

    pieces = []
    for tile in range(2):
        pieces.append(sources[:, tile * rows_p : (tile + 1) * rows_p, :].reshape(depth, LANES).T)
    piece = jnp.concatenate(pieces, axis=0)
    high = piece.astype(jnp.bfloat16)
    low = (piece - high.astype(jnp.float32)).astype(jnp.bfloat16)
    result = jnp.dot(high, table_high[...], preferred_element_type=jnp.float32)
    result += jnp.dot(low, table_high[...], preferred_element_type=jnp.float32)
    result += jnp.dot(high, table_low[...], preferred_element_type=jnp.float32)
    if has_previous:
        result += previous[...]
    if final:
        for i in range(group_rows):
            out[i] = result[i * members : (i + 1) * members]
    else:
        out[...] = result


def synthesis(tables, sources, previous, final, groups, group_rows, members):
    depth, length = tables[0].shape

    def body(*refs):
        synthesis_kernel(previous is not None, final, groups, group_rows, members, *refs)

    rows_p = depth // sources.shape[0]
    table = pl.BlockSpec((depth, length), lambda b: (0, 0))
    partial = pl.BlockSpec((2 * LANES, length), lambda b: (b, 0))
    in_specs = [table, table, pl.BlockSpec((sources.shape[0], 2 * rows_p, LANES), lambda b: (0, b, 0))]
    space = pltpu.VMEM if final and sources.size < 2**19 else pltpu.HBM
    args = [pltpu.with_memory_space_constraint(part, space) for part in tables]
    args.append(pltpu.with_memory_space_constraint(sources, space))
    if previous is not None:
        in_specs.append(partial)
        args.append(pltpu.with_memory_space_constraint(previous, pltpu.HBM))
    if final:
        out_spec = pl.BlockSpec((group_rows, members, length), lambda b: (b, 0, 0))
        out_shape = jax.ShapeDtypeStruct((groups * group_rows, members, length), jnp.float32)
    else:
        out_spec = partial
        out_shape = pltpu.HBM((groups * 2 * LANES, length), jnp.float32)
    return pl.pallas_call(
        body,
        grid=(groups,),
        in_specs=in_specs,
        out_specs=out_spec,
        out_shape=out_shape,
        compiler_params=pltpu.CompilerParams(
            dimension_semantics=("arbitrary",), vmem_limit_bytes=26 * 2**20
        ),
        cost_estimate=pl.CostEstimate(
            flops=6 * groups * 256 * depth * length, bytes_accessed=12 * 10**6, transcendentals=0
        ),
        name="synthesis",
    )(*args)


def synthesis_tables(waves, parts, length):
    count, slots = waves.shape
    numbers = []
    for start, size in parts:
        rows = jnp.repeat(waves[:, start : start + size], 2, axis=1)
        pad = round_up(2 * size, 8) - 2 * size
        numbers.append(jnp.pad(rows, ((0, 0), (0, pad)), constant_values=-1).reshape(-1))
    number = jnp.concatenate(numbers)[:, None]
    lane = lax.broadcasted_iota(jnp.int32, (number.shape[0], LANES), 1)
    part = lax.broadcasted_iota(jnp.int32, (number.shape[0], LANES), 0) % 2
    weight = jnp.where(number == 0, 1.0, jnp.where(number < 0, 0.0, 2.0)).astype(jnp.float32)
    wave = jnp.maximum(number, 0)
    near = ((wave * lane + part * (length // 4)) % length).astype(jnp.float32) * (TWO_PI / length)
    far = ((wave * (lane * LANES % length)) % length).astype(jnp.float32) * (TWO_PI / length)
    fine = jnp.stack([weight * jnp.cos(near), weight * jnp.sin(near)])
    coarse = jnp.stack([jnp.cos(far), jnp.sin(far)])
    return fine, coarse


def local(coeffs_old, noise, legendre, decay, amplitude, wavenumber_of_slot, lat_order):
    lat_count = lax.axis_size("lat")
    lon_count = lax.axis_size("lon")
    count = lat_count * lon_count
    me = lax.axis_index("lat") * lon_count + lax.axis_index("lon")
    shape = coeffs_old.shape
    slots, _, scales, members, width = shape
    latitudes = lat_order.shape[0]
    rows = latitudes // count
    group_rows = (2 * LANES) // members
    while rows % group_rows:
        group_rows -= 1
    groups = rows // group_rows

    order = lat_order.reshape(-1, LANES)
    base = (me * slots).reshape(1).astype(jnp.int32)

    old = dense(coeffs_old)
    fresh_noise = dense(noise)
    parts = chunks_of(slots)
    last = len(parts) - 1
    depths = [count * round_up(2 * size, 8) for _, size in parts]
    new = None
    pattern = None
    received = []
    tables = []
    for index, (start, size) in enumerate(parts):
        new, messages = spectral(
            old, fresh_noise, legendre, amplitude, decay, wavenumber_of_slot, base, order, shape,
            start, size, index > 0 or last == 0, new, count, groups, group_rows,
        )
        if index == 0:
            messages, waves = lax.optimization_barrier((messages, wavenumber_of_slot))
            fine, coarse = synthesis_tables(waves.reshape(count, slots), parts, LON)
            tables = [
                expand_tables(fine, coarse, sum(depths[:i]), depths[i], LON) for i in range(len(parts))
            ]
        if index == 2:
            pattern = synthesis(
                tables[0], received[0], None, False, groups, group_rows, members
            )
        if index == last and index:
            new = update(
                old, fresh_noise, amplitude, decay, wavenumber_of_slot, base, shape, *parts[0], new
            )
            messages, pattern, tables, new = lax.optimization_barrier(
                (messages, pattern, tables, new)
            )
        received.append(lax.all_to_all(messages, AXES, 0, 0, tiled=True))
    for index in range(1 if last >= 2 else 0, len(parts)):
        pattern = synthesis(
            tables[index], received[index], pattern, index == last,
            groups, group_rows, members,
        )
    return (undense(new, shape), pattern)


def solution(mesh):
    in_specs = (
        P(AXES, None, None, None, None),
        P(AXES, None, None, None, None),
        P(AXES, None, None),
        P(),
        P(),
        P(),
        P(),
    )
    out_specs = (P(AXES, None, None, None, None), P(AXES, None, None))
    return jax.shard_map(local, mesh=mesh, in_specs=in_specs, out_specs=out_specs, check_vma=False)
```
